32 devices in a mesh: gx: 4 (over y, core), gy: 8 (over z, x).
Axes of the slice: x: 2, y: 2, z: 4, core: 2. Of those that a mesh axis runs over, the one named last changes fastest.
Arguments:
- emission: float32 [512, 8, 128], P(('gx', 'gy')), may hold values from 0.05 to 1
- reflectance: float32 [512, 8, 128], P(('gx', 'gy')), may hold values from 0.5 to 0.98
- form_factors: float32 [8192, 128, 128], P(('gx', 'gy')), as said below
- link_source: int32 [8192], P(('gx', 'gy')), may hold values from 0 to 511, as said below
- link_target: int32 [8192], P(('gx', 'gy')), may hold values from 0 to 511, as said below
- link_length: int32 [8192], P(('gx', 'gy')), may hold values from 32 to 128
- block_count: int32 [32], P(('gx', 'gy')), may hold values from 32 to 256, as said below
Outputs:
- solution: float32 [512, 8, 128], P(('gx', 'gy'))
- residual: float32 [512, 8, 128], P(('gx', 'gy'))
The draws below stay inside these ranges and needn't reach their ends.
Inputs may be any that keep to these rules, and one draw needn't show every extreme that they name: `form_factors`: entries are nonnegative. `link_source`: block k's source is any cluster; among the blocks held by one device, all blocks whose sources lie on one same device name the same source cluster. `link_target`: block k's target is one of the clusters of the device holding it, clusters (k // 256) * 16 to (k // 256) * 16 + 15. `block_count`: some device has all 256 slots live.
All inputs are finite; a program needn't handle non-finite values.
Results may differ from the reference program's by a relative error of at most 0.0011.
Values sent between devices are 32-bit elements; how exact they have to be, the bound alone decides.
A program may use at most 64 MiB of HBM per device.

```python
import math
import jax
import jax.numpy as jnp
from jax import lax

CL = 128
BANDS = 8
CPD = 16
BLK_DEV = 256
ITERS = 3
NCL = 512
NBLK = 8192
DEVICES = 32


def count_table(key):
    roll_draw = jax.random.randint(jax.random.fold_in(key, 11), (DEVICES,), 0, 8)
    least_count = max(1, BLK_DEV // 8)
    counts = least_count + (BLK_DEV - least_count) * (roll_draw * roll_draw * roll_draw) // 343
    full_dev = jax.random.randint(jax.random.fold_in(key, 12), (), 0, DEVICES)
    return jnp.where(jnp.arange(DEVICES, dtype=jnp.int32) == full_dev, BLK_DEV, counts).astype(jnp.int32)


def draw_block_count(key, part):
    return count_table(key)


def draw_link_source(key, part):
    block_ids = jnp.arange(NBLK, dtype=jnp.int32)
    holder = block_ids // BLK_DEV
    slot_index = block_ids % BLK_DEV
    random_peer = jax.random.randint(jax.random.fold_in(key, 21), (NBLK,), 0, DEVICES)
    far_peer = (holder + DEVICES // 2) % DEVICES
    next_peer = (holder + 1) % DEVICES
    peer_dev = jnp.where(slot_index == 0, far_peer, jnp.where(slot_index == 1, next_peer, random_peer))
    stride_draw = jax.random.randint(jax.random.fold_in(key, 22), (2,), 0, CPD)
    slot_pick = 1 + (holder + peer_dev * (2 * stride_draw[0] + 1) + stride_draw[1]) % (CPD - 1)
    return (peer_dev * CPD + slot_pick).astype(jnp.int32)


def draw_link_target(key, part):
    holder = jnp.arange(NBLK, dtype=jnp.int32) // BLK_DEV
    local_pick = jax.random.randint(jax.random.fold_in(key, 23), (NBLK,), 0, CPD)
    return (holder * CPD + local_pick).astype(jnp.int32)


def draw_form_factors(key, part):
    counts = count_table(key)
    holder = jnp.arange(NBLK, dtype=jnp.int32) // BLK_DEV
    block_scale = 1.4 * CPD / (counts[holder].astype(jnp.float32) * CL)
    uniform_draw = jax.random.uniform(jax.random.fold_in(key, 31), (NBLK, CL, CL), jnp.float32)
    return uniform_draw * block_scale[:, None, None]


def place_ends(array, rng, least, high):
    spot = [jax.random.randint(jax.random.fold_in(rng, axis), (), 0, length) for axis, length in enumerate(array.shape)]
    longest = array.shape.index(max(array.shape))
    next_to = spot[:longest] + [(spot[longest] + 1) % array.shape[longest]] + spot[longest + 1:]
    return array.at[tuple(spot)].set(least).at[tuple(next_to)].set(high)


def level_of(own_key, extent, shards, smallest, top_value):
    gain, own = 1.0, jax.random.fold_in(own_key, 6)
    for position, shards_of in shards:
        heights = jnp.exp(jax.random.uniform(jax.random.fold_in(own, position), (shards_of,), jnp.float32, smallest / len(shards), top_value / len(shards)))
        gain = gain * jnp.repeat(heights, extent[position] // shards_of).reshape([-1 if axis == position else 1 for axis in range(len(extent))])
    return gain


def setup_inputs(seed: int = 0) -> dict:
    key_of = jax.random.split(jax.random.key(seed), 8)
    emission = jnp.clip(jnp.exp(math.log(1.0) - 2.9957323 * jax.random.uniform(key_of[0], (NCL, BANDS, CL), jnp.float32) ** level_of(key_of[0], (NCL, BANDS, CL), ((0, 32),), -0.2, 0.2)), 0.05, 1.0)
    reflectance = jnp.clip(jnp.exp(math.log(0.98) - 0.6729445 * jax.random.uniform(key_of[1], (NCL, BANDS, CL), jnp.float32) ** level_of(key_of[1], (NCL, BANDS, CL), ((0, 32),), -0.2, 0.2)), 0.5, 0.98)
    form_factors = draw_form_factors(jax.random.fold_in(key_of[7], 71), 0)
    link_source = draw_link_source(jax.random.fold_in(key_of[7], 71), 0)
    link_target = draw_link_target(jax.random.fold_in(key_of[7], 71), 0)
    link_length = place_ends(jax.random.randint(key_of[5], (NBLK,), CL // 4, CL + 1), jax.random.fold_in(key_of[5], 1), CL // 4, CL).astype(jnp.int32)
    block_count = draw_block_count(jax.random.fold_in(key_of[7], 71), 0)
    return dict(emission=emission, reflectance=reflectance, form_factors=form_factors, link_source=link_source, link_target=link_target, link_length=link_length, block_count=block_count)


def apply_operator(radiance, reflectance, form_factors, link_source, link_target, link_length, block_count):
    column_ids = jnp.arange(CL, dtype=jnp.int32)
    slot_ids = jnp.arange(BLK_DEV, dtype=jnp.int32)
    float_type = radiance.dtype

    def per_device(total, inputs):
        factors, source_ids, target_ids, lengths, live_count = inputs
        live_block = slot_ids < live_count
        column_mask = ((column_ids[None, :] < lengths[:, None]) & live_block[:, None]).astype(float_type)
        source_vals = radiance[source_ids] * column_mask[:, None, :]
        partial_sum = jnp.einsum("kij,kbj->kbi", factors, source_vals, precision=lax.Precision.HIGHEST)
        total = total + jax.ops.segment_sum(partial_sum, target_ids, num_segments=NCL)
        return total, None

    inputs = (form_factors.reshape(DEVICES, BLK_DEV, CL, CL),
              link_source.reshape(DEVICES, BLK_DEV),
              link_target.reshape(DEVICES, BLK_DEV),
              link_length.reshape(DEVICES, BLK_DEV),
              block_count)
    gathered, _ = lax.scan(per_device, jnp.zeros_like(radiance), inputs)
    return radiance - reflectance * gathered


def reference(emission, reflectance, form_factors, link_source, link_target, link_length, block_count):
    def operate(radiance):
        return apply_operator(radiance, reflectance, form_factors, link_source, link_target, link_length, block_count)

    float_type = emission.dtype
    solution = jnp.zeros_like(emission)
    residual = emission
    shadow = emission
    direction = jnp.zeros_like(emission)
    applied = jnp.zeros_like(emission)
    rho_old = jnp.ones((), float_type)
    alpha_coef = jnp.ones((), float_type)
    omega_coef = jnp.ones((), float_type)
    for iteration in range(ITERS):
        rho_new = jnp.sum(shadow * residual)
        beta_coef = (rho_new / rho_old) * (alpha_coef / omega_coef)
        direction = residual + beta_coef * (direction - omega_coef * applied)
        applied = operate(direction)
        alpha_coef = rho_new / jnp.sum(shadow * applied)
        middle = residual - alpha_coef * applied
        bounce = operate(middle)
        omega_coef = jnp.sum(bounce * middle) / jnp.sum(bounce * bounce)
        solution = solution + alpha_coef * direction + omega_coef * middle
        residual = middle - omega_coef * bounce
        rho_old = rho_new
    return solution, residual
```

```python
import jax
import jax.numpy as jnp
from jax import lax
from jax.sharding import PartitionSpec as P
from jax.experimental import pallas as pl
from jax.experimental.pallas import tpu as pltpu

ITERS = 3
PHASES = 2 * ITERS + 1
CHUNK = 16
SLOTS = 4
UNROLL = 16


def kernel(perm_s, own_s, len_s, keep_s, end_s, val_s, want_s, em, refl, ff, sol, res,
           w, stage, runs, vt, outb, inb, dout, din, image, direction, total, rs, ds, ims,
           stage_sem, send_sem, recv_sem, dsend_sem, drecv_sem):
    nx, ny = lax.axis_size("gx"), lax.axis_size("gy")
    n = nx * ny
    me = lax.axis_index("gx") * ny + lax.axis_index("gy")
    clusters = em.shape[0]
    blocks, cl = ff.shape[0], ff.shape[2]
    chunks = blocks // CHUNK
    f32, bf16 = jnp.float32, jnp.bfloat16

    def fetch(c, slot):
        return pltpu.make_async_copy(ff.at[pl.ds(c * CHUNK, CHUNK)], stage.at[slot], stage_sem.at[slot])

    for c in range(min(SLOTS, chunks)):
        fetch(c, c).start()

    barrier = pltpu.get_barrier_semaphore()

    def greet(r, carry):
        peer = lax.rem(me + r, n)
        pl.semaphore_signal(barrier, inc=1, device_id=(peer // ny, lax.rem(peer, ny)),
                            device_id_type=pl.DeviceIdType.MESH)
        return carry

    lax.fori_loop(1, n, greet, 0)
    pl.semaphore_wait(barrier, n - 1)

    lane = lax.broadcasted_iota(jnp.int32, (1, 128), 1)

    def dot(a, b):
        part = jnp.sum(a * b, axis=0)
        part = jnp.sum(part, axis=0, keepdims=True)
        return jnp.sum(part, axis=1, keepdims=True)

    def send(phase, field, pairs):
        if field is not None:
            def one(r, carry):
                peer = lax.rem(me + r, n)
                outb[phase, peer] = field[want_s[peer]]
                pltpu.make_async_remote_copy(
                    src_ref=outb.at[phase, peer], dst_ref=inb.at[phase, me],
                    send_sem=send_sem.at[phase], recv_sem=recv_sem.at[phase],
                    device_id=(peer // ny, lax.rem(peer, ny)),
                    device_id_type=pl.DeviceIdType.MESH).start()
                return carry

            lax.fori_loop(1, n, one, 0)
            inb[phase, me] = field[want_s[me]]
        row = jnp.zeros((1, 128), f32)
        for i, (a, b) in enumerate(pairs):
            row = jnp.where(lane == i, jnp.broadcast_to(dot(a[...], b[...]), (1, 128)), row)
        dout[phase] = row
        din[phase, me] = row

        def two(r, carry):
            peer = lax.rem(me + r, n)
            pltpu.make_async_remote_copy(
                src_ref=dout.at[phase], dst_ref=din.at[phase, me],
                send_sem=dsend_sem.at[phase], recv_sem=drecv_sem.at[phase],
                device_id=(peer // ny, lax.rem(peer, ny)),
                device_id_type=pl.DeviceIdType.MESH).start()
            return carry

        lax.fori_loop(1, n, two, 0)

    def drain(ref, sem):
        part = ref.at[pl.ds(0, n - 1)]
        pltpu.make_async_copy(part, part, sem).wait()

    def receive(phase, count, rows):
        drain(din.at[phase], drecv_sem.at[phase])
        drain(din.at[phase], dsend_sem.at[phase])
        sums = jnp.sum(din[phase], axis=0)
        if rows:
            drain(inb.at[phase], recv_sem.at[phase])
            drain(outb.at[phase], send_sem.at[phase])
        return [jnp.broadcast_to(jnp.sum(jnp.where(lane == i, sums, 0.0), axis=1, keepdims=True), (8, 128))
                for i in range(count)]

    def put_sources(v):
        low = v - v.astype(bf16).astype(f32)
        vt[...] = jnp.concatenate([v, low], axis=1).astype(bf16)

    def apply(v):
        def step(s, acc):
            for u in range(UNROLL // 2):
                r = s * UNROLL + 2 * u
                va, vb = vt[own_s[r]], vt[own_s[r + 1]]
                left = jnp.concatenate([jnp.concatenate([va, va], axis=1),
                                        jnp.concatenate([vb, vb], axis=1)], axis=0)
                right = jnp.concatenate([w[perm_s[r]], w[perm_s[r + 1]]], axis=1)
                out = jnp.dot(left, right, preferred_element_type=f32)
                acc = acc * keep_s[r] + (out[0:8, :cl] + out[8:16, :cl])
                runs[r] = acc
                acc = acc * keep_s[r + 1] + (out[16:24, cl:] + out[24:32, cl:])
                runs[r + 1] = acc
            return acc

        lax.fori_loop(0, blocks // UNROLL, step, jnp.zeros((8, cl), f32))
        g = jnp.stack([runs[end_s[t]] * val_s[t] for t in range(clusters)])
        return v - refl[...] * g

    send(0, em, [(em, em)])

    def prepare(c, carry):
        slot = lax.rem(c, SLOTS)
        fetch(c, slot).wait()

        def block(b, inner):
            k = c * CHUNK + b
            t = stage[slot, b].T
            j = lax.broadcasted_iota(jnp.int32, (cl, cl), 0)
            t = jnp.where(j < len_s[k], t, 0.0)
            high = t.astype(bf16)
            w[k, 0:cl] = high
            w[k, cl:2 * cl] = (t - high.astype(f32)).astype(bf16)
            return inner

        lax.fori_loop(0, CHUNK, block, 0, unroll=4)

        @pl.when(c + SLOTS < chunks)
        def _():
            fetch(c + SLOTS, slot).start()

        return carry

    lax.fori_loop(0, chunks, prepare, 0)

    (rho,) = receive(0, 1, True)
    rs[...] = inb[0]
    res[...] = em[...]
    rho_old, alpha, omega = None, None, None
    for it in range(ITERS):
        last = it == ITERS - 1
        if it == 0:
            direction[...] = em[...]
            ds[...] = rs[...]
        else:
            beta = rho / rho_old * (alpha / omega)
            direction[...] = res[...] + beta * (direction[...] - omega * image[...])
            ds[...] = rs[...] + beta * (ds[...] - omega * ims[...])
        put_sources(ds[...])
        image[...] = apply(direction[...])
        phase = 1 + 2 * it
        send(phase, image, [(em, image)])
        (sim,) = receive(phase, 1, True)
        alpha = rho / sim
        ims[...] = inb[phase]
        res[...] = res[...] - alpha * image[...]
        rs[...] = rs[...] - alpha * ims[...]
        put_sources(rs[...])
        sol[...] = apply(res[...])
        send(phase + 1, None if last else sol, [(sol, res), (sol, sol), (em, res), (em, sol)])
        cross, square, sm, sb = receive(phase + 1, 4, not last)
        omega = cross / square
        if it == 0:
            total[...] = alpha * direction[...] + omega * res[...]
        else:
            total[...] = total[...] + alpha * direction[...] + omega * res[...]
        res[...] = res[...] - omega * sol[...]
        if not last:
            rs[...] = rs[...] - omega * inb[phase + 1]
        rho_old = rho
        rho = sm - omega * sb
    sol[...] = total[...]


def local(emission, reflectance, form_factors, link_source, link_target, link_length, block_count):
    clusters, bands, cl = emission.shape
    blocks = form_factors.shape[0]
    devices = lax.axis_size(("gx", "gy"))
    i32, f32, bf16 = jnp.int32, jnp.float32, jnp.bfloat16
    ids = jnp.arange(blocks, dtype=i32)
    live = ids < block_count[0]
    owner = link_source // clusters
    slot = link_source % clusters
    peers = jnp.arange(devices, dtype=i32)
    match = (owner[None, :] == peers[:, None]) & live[None, :]
    wanted = jnp.max(jnp.where(match, slot[None, :], 0), axis=1)
    want = lax.all_to_all(wanted, ("gx", "gy"), split_axis=0, concat_axis=0, tiled=True)
    length = jnp.where(live, link_length, 0)
    target = link_target % clusters
    key = target * blocks + ids
    rank = jnp.sum((key[None, :] < key[:, None]).astype(i32), axis=1)
    place = rank[None, :] == ids[:, None]
    perm = jnp.sum(jnp.where(place, ids[None, :], 0), axis=1)
    own = jnp.sum(jnp.where(place, owner[None, :], 0), axis=1)
    sorted_target = jnp.sum(jnp.where(place, target[None, :], 0), axis=1)
    before = jnp.concatenate([jnp.full((1,), -1, i32), sorted_target[:-1]])
    keep = (before == sorted_target).astype(f32)
    cids = jnp.arange(clusters, dtype=i32)
    end = jnp.maximum(jnp.sum((target[None, :] <= cids[:, None]).astype(i32), axis=1) - 1, 0)
    valid = jnp.any(target[None, :] == cids[:, None], axis=1).astype(f32)
    smem = pl.BlockSpec(memory_space=pltpu.SMEM)
    vmem = pl.BlockSpec(memory_space=pltpu.VMEM)
    field = (clusters, bands, cl)
    rows = (devices, bands, cl)
    dma = pltpu.SemaphoreType.DMA
    return pl.pallas_call(
        kernel,
        out_shape=[jax.ShapeDtypeStruct(field, f32)] * 2,
        in_specs=[smem] * 7 + [vmem, vmem, pl.BlockSpec(memory_space=pl.ANY)],
        out_specs=[vmem, vmem],
        scratch_shapes=[
            pltpu.VMEM((blocks, 2 * cl, cl), bf16),
            pltpu.VMEM((SLOTS, CHUNK, cl, cl), f32),
            pltpu.VMEM((blocks, bands, cl), f32),
            pltpu.VMEM((devices, 2 * bands, cl), bf16),
            pltpu.VMEM((PHASES - 1,) + rows, f32),
            pltpu.VMEM((PHASES - 1,) + rows, f32),
            pltpu.VMEM((PHASES, 1, 128), f32),
            pltpu.VMEM((PHASES, devices, 1, 128), f32),
            pltpu.VMEM(field, f32),
            pltpu.VMEM(field, f32),
            pltpu.VMEM(field, f32),
            pltpu.VMEM(rows, f32),
            pltpu.VMEM(rows, f32),
            pltpu.VMEM(rows, f32),
            dma((SLOTS,)),
            dma((PHASES,)),
            dma((PHASES,)),
            dma((PHASES,)),
            dma((PHASES,)),
        ],
        compiler_params=pltpu.CompilerParams(
            collective_id=0, has_side_effects=True, vmem_limit_bytes=56 * 1024 * 1024),
        name="radiosity",
    )(perm, own, length, keep, end, valid, want, emission, reflectance, form_factors)


def solution(mesh):
    wide = P(("gx", "gy"), None, None)
    flat = P(("gx", "gy"))
    return jax.shard_map(local, mesh=mesh, in_specs=(wide, wide, wide, flat, flat, flat, flat),
                         out_specs=(wide, wide), check_vma=False)
```

```python
import jax
import jax.numpy as jnp
from jax import lax
from jax.sharding import PartitionSpec as P
from jax.experimental import pallas as pl
from jax.experimental.pallas import tpu as pltpu

ITERS = 3
PHASES = 2 * ITERS + 1
CHUNK = 16
SLOTS = 4
UNROLL = 64
EARLY = 4


def divide(x, by):
    if by & (by - 1) == 0:
        return lax.shift_right_logical(x, by.bit_length() - 1), lax.bitwise_and(x, by - 1)
    return lax.div(x, by), lax.rem(x, by)


def kernel(len_s, count_s, source_v, target_v, count_v, em, refl, ff, sol, res,
           w, stage, runs, vt, outb, inb, dout, din, image, direction, total, rs, ds, ims,
           wout, win, want_s, ints_v, ints_s, reals_v, reals_s,
           stage_sem, send_sem, recv_sem, dsend_sem, drecv_sem, wsend_sem, wrecv_sem, small_sem):
    nx, ny = lax.axis_size("gx"), lax.axis_size("gy")
    n = nx * ny
    me = lax.axis_index("gx") * ny + lax.axis_index("gy")
    clusters = em.shape[0]
    blocks, cl = ff.shape[0], ff.shape[2]
    chunks = blocks // CHUNK
    f32, bf16 = jnp.float32, jnp.bfloat16

    def fetch(c, slot):
        return pltpu.make_async_copy(ff.at[pl.ds(c * CHUNK, CHUNK)], stage.at[slot], stage_sem.at[slot])

    for c in range(min(SLOTS, chunks)):
        fetch(c, c).start()

    barrier = pltpu.get_barrier_semaphore()

    def greet(r, carry):
        peer = lax.rem(me + r, n)
        pl.semaphore_signal(barrier, inc=1, device_id=(peer // ny, lax.rem(peer, ny)),
                            device_id_type=pl.DeviceIdType.MESH)
        return carry

    lax.fori_loop(1, n, greet, 0)

    i32 = jnp.int32
    owner, slot = divide(source_v[...], clusters)
    target = target_v[...] - me * clusters
    ids = lax.broadcasted_iota(i32, (1, blocks), 1)
    peers = lax.broadcasted_iota(i32, (n, blocks), 0)
    alive = jnp.broadcast_to(ids < count_v[:, 0:1], (n, blocks))
    match = jnp.logical_and(owner == peers, alive)
    wanted = jnp.max(jnp.where(match, jnp.broadcast_to(slot, (n, blocks)), 0), axis=1, keepdims=True)
    wout[...] = jnp.broadcast_to(wanted, (n, 128)).reshape(n, 1, 128)
    pl.semaphore_wait(barrier, n - 1)

    def ask(r, carry):
        peer = lax.rem(me + r, n)
        pltpu.make_async_remote_copy(
            src_ref=wout.at[peer], dst_ref=win.at[me], send_sem=wsend_sem, recv_sem=wrecv_sem,
            device_id=(peer // ny, lax.rem(peer, ny)),
            device_id_type=pl.DeviceIdType.MESH).start()
        return carry

    lax.fori_loop(1, n, ask, 0)
    win[me] = wout[me]

    square_of = (blocks, blocks)
    down = lax.broadcasted_iota(i32, square_of, 0)
    across = lax.broadcasted_iota(i32, square_of, 1)

    def upright(row):
        return jnp.sum(jnp.where(down == across, jnp.broadcast_to(row, square_of), 0), axis=1, keepdims=True)

    key = target * blocks + ids
    key_up, owner_up, target_up = upright(key), upright(owner), upright(target)
    rank = jnp.sum((jnp.broadcast_to(key, square_of) < key_up).astype(i32), axis=1, keepdims=True)
    placed = rank == across

    def ordered(column):
        return jnp.sum(jnp.where(placed, column, 0), axis=0, keepdims=True)

    sorted_target = ordered(jnp.broadcast_to(target_up, square_of))
    ints_v[...] = jnp.zeros(ints_v.shape, i32)
    reals_v[...] = jnp.zeros(reals_v.shape, f32)
    ints_v[0:1, :] = ordered(down)
    ints_v[1:2, :] = ordered(jnp.broadcast_to(owner_up, square_of))
    up_to = jnp.sum((target_up <= across).astype(i32), axis=0, keepdims=True)
    same = jnp.sum((target_up == across).astype(i32), axis=0, keepdims=True)
    ints_v[2:3, :] = jnp.maximum(up_to - 1, 0)
    shifted = pltpu.roll(jnp.broadcast_to(sorted_target, (8, blocks)), 1, 1)[0:1]
    joined = jnp.logical_and(shifted == sorted_target, ids > 0)
    reals_v[0:1, :] = jnp.where(joined, 1.0, 0.0)
    reals_v[1:2, :] = jnp.where(same > 0, 1.0, 0.0)
    small = (pltpu.make_async_copy(ints_v, ints_s, small_sem.at[0]),
             pltpu.make_async_copy(reals_v, reals_s, small_sem.at[1]))
    for copy in small:
        copy.start()

    lane = lax.broadcasted_iota(jnp.int32, (1, 128), 1)

    def dot(a, b):
        part = jnp.sum(a * b, axis=0)
        part = jnp.sum(part, axis=0, keepdims=True)
        return jnp.sum(part, axis=1, keepdims=True)

    def send(phase, field, pairs):
        if field is not None:
            def one(r, carry):
                peer = lax.rem(me + r, n)
                outb[phase, peer] = field[want_s[peer, 0, 0]]
                pltpu.make_async_remote_copy(
                    src_ref=outb.at[phase, peer], dst_ref=inb.at[phase, me],
                    send_sem=send_sem.at[phase], recv_sem=recv_sem.at[phase],
                    device_id=(peer // ny, lax.rem(peer, ny)),
                    device_id_type=pl.DeviceIdType.MESH).start()
                return carry

            lax.fori_loop(1, n, one, 0)
            inb[phase, me] = field[want_s[me, 0, 0]]
        row = jnp.zeros((1, 128), f32)
        for i, (a, b) in enumerate(pairs):
            row = jnp.where(lane == i, jnp.broadcast_to(dot(a[...], b[...]), (1, 128)), row)
        dout[phase] = row
        din[phase, me] = row

        def two(r, carry):
            peer = lax.rem(me + r, n)
            pltpu.make_async_remote_copy(
                src_ref=dout.at[phase], dst_ref=din.at[phase, me],
                send_sem=dsend_sem.at[phase], recv_sem=drecv_sem.at[phase],
                device_id=(peer // ny, lax.rem(peer, ny)),
                device_id_type=pl.DeviceIdType.MESH).start()
            return carry

        lax.fori_loop(1, n, two, 0)

    def drain(ref, sem):
        part = ref.at[pl.ds(0, n - 1)]
        pltpu.make_async_copy(part, part, sem).wait()

    def receive(phase, count, rows):
        drain(din.at[phase], drecv_sem.at[phase])
        drain(din.at[phase], dsend_sem.at[phase])
        sums = jnp.sum(din[phase], axis=0)
        if rows:
            drain(inb.at[phase], recv_sem.at[phase])
            drain(outb.at[phase], send_sem.at[phase])
        return [jnp.broadcast_to(jnp.sum(jnp.where(lane == i, sums, 0.0), axis=1, keepdims=True), (8, 128))
                for i in range(count)]

    def put_sources(v):
        low = v - v.astype(bf16).astype(f32)
        vt[...] = jnp.concatenate([v, low], axis=1).astype(bf16)

    def apply(v):
        def step(s, acc):
            for u in range(UNROLL // 2):
                r = s * UNROLL + 2 * u
                va, vb = vt[ints_s[1, r]], vt[ints_s[1, r + 1]]
                left = jnp.concatenate([jnp.concatenate([va, va], axis=1),
                                        jnp.concatenate([vb, vb], axis=1)], axis=0)
                right = jnp.concatenate([w[ints_s[0, r]], w[ints_s[0, r + 1]]], axis=1)
                out = jnp.dot(left, right, preferred_element_type=f32)
                acc = acc * reals_s[0, r] + (out[0:8, :cl] + out[8:16, :cl])
                runs[r] = acc
                acc = acc * reals_s[0, r + 1] + (out[16:24, cl:] + out[24:32, cl:])
                runs[r + 1] = acc
            return acc

        lax.fori_loop(0, blocks // UNROLL, step, jnp.zeros((8, cl), f32))
        g = jnp.stack([runs[ints_s[2, t]] * reals_s[1, t] for t in range(clusters)])
        return v - refl[...] * g

    def prepare(c, carry):
        slot = lax.rem(c, SLOTS)
        fetch(c, slot).wait()

        def block(b, inner):
            k = c * CHUNK + b
            t = stage[slot, b].T
            j = lax.broadcasted_iota(jnp.int32, (cl, cl), 0)
            t = jnp.where(j < jnp.where(k < count_s[0], len_s[k], 0), t, 0.0)
            high = t.astype(bf16)
            w[k, 0:cl] = high
            w[k, cl:2 * cl] = (t - high.astype(f32)).astype(bf16)
            return inner

        lax.fori_loop(0, CHUNK, block, 0, unroll=4)

        @pl.when(c + SLOTS < chunks)
        def _():
            fetch(c + SLOTS, slot).start()

        return carry

    early = min(EARLY, chunks)
    lax.fori_loop(0, early, prepare, 0)
    drain(win, wrecv_sem)
    drain(wout, wsend_sem)
    asked = pltpu.make_async_copy(win, want_s, small_sem.at[2])
    asked.start()
    asked.wait()
    send(0, em, [(em, em)])
    lax.fori_loop(early, chunks, prepare, 0)
    for copy in small:
        copy.wait()

    (rho,) = receive(0, 1, True)
    rs[...] = inb[0]
    res[...] = em[...]
    rho_old, alpha, omega = None, None, None
    for it in range(ITERS):
        last = it == ITERS - 1
        if it == 0:
            direction[...] = em[...]
            ds[...] = rs[...]
        else:
            beta = rho / rho_old * (alpha / omega)
            direction[...] = res[...] + beta * (direction[...] - omega * image[...])
            ds[...] = rs[...] + beta * (ds[...] - omega * ims[...])
        put_sources(ds[...])
        image[...] = apply(direction[...])
        phase = 1 + 2 * it
        send(phase, image, [(em, image)])
        (sim,) = receive(phase, 1, True)
        alpha = rho / sim
        ims[...] = inb[phase]
        res[...] = res[...] - alpha * image[...]
        rs[...] = rs[...] - alpha * ims[...]
        put_sources(rs[...])
        sol[...] = apply(res[...])
        send(phase + 1, None if last else sol, [(sol, res), (sol, sol), (em, res), (em, sol)])
        cross, square, sm, sb = receive(phase + 1, 4, not last)
        omega = cross / square
        if it == 0:
            total[...] = alpha * direction[...] + omega * res[...]
        else:
            total[...] = total[...] + alpha * direction[...] + omega * res[...]
        res[...] = res[...] - omega * sol[...]
        if not last:
            rs[...] = rs[...] - omega * inb[phase + 1]
        rho_old = rho
        rho = sm - omega * sb
    sol[...] = total[...]


def local(emission, reflectance, form_factors, link_source, link_target, link_length, block_count):
    clusters, bands, cl = emission.shape
    blocks = form_factors.shape[0]
    devices = lax.axis_size(("gx", "gy"))
    i32, f32, bf16 = jnp.int32, jnp.float32, jnp.bfloat16
    smem = pl.BlockSpec(memory_space=pltpu.SMEM)
    vmem = pl.BlockSpec(memory_space=pltpu.VMEM)
    field = (clusters, bands, cl)
    rows = (devices, bands, cl)
    dma = pltpu.SemaphoreType.DMA
    return pl.pallas_call(
        kernel,
        out_shape=[jax.ShapeDtypeStruct(field, f32)] * 2,
        in_specs=[smem] * 2 + [vmem] * 5 + [pl.BlockSpec(memory_space=pl.ANY)],
        out_specs=[vmem, vmem],
        scratch_shapes=[
            pltpu.VMEM((blocks, 2 * cl, cl), bf16),
            pltpu.VMEM((SLOTS, CHUNK, cl, cl), f32),
            pltpu.VMEM((blocks, bands, cl), f32),
            pltpu.VMEM((devices, 2 * bands, cl), bf16),
            pltpu.VMEM((PHASES - 1,) + rows, f32),
            pltpu.VMEM((PHASES - 1,) + rows, f32),
            pltpu.VMEM((PHASES, 1, 128), f32),
            pltpu.VMEM((PHASES, devices, 1, 128), f32),
            pltpu.VMEM(field, f32),
            pltpu.VMEM(field, f32),
            pltpu.VMEM(field, f32),
            pltpu.VMEM(rows, f32),
            pltpu.VMEM(rows, f32),
            pltpu.VMEM(rows, f32),
            pltpu.VMEM((devices, 1, 128), i32),
            pltpu.VMEM((devices, 1, 128), i32),
            pltpu.SMEM((devices, 1, 128), i32),
            pltpu.VMEM((8, blocks), i32),
            pltpu.SMEM((8, blocks), i32),
            pltpu.VMEM((8, blocks), f32),
            pltpu.SMEM((8, blocks), f32),
            dma((SLOTS,)),
            dma((PHASES,)),
            dma((PHASES,)),
            dma((PHASES,)),
            dma((PHASES,)),
            dma,
            dma,
            dma((3,)),
        ],
        compiler_params=pltpu.CompilerParams(
            collective_id=0, has_side_effects=True, vmem_limit_bytes=56 * 1024 * 1024),
        name="radiosity",
    )(link_length, block_count, link_source.reshape(1, blocks), link_target.reshape(1, blocks),
      block_count.reshape(1, 1), emission, reflectance, form_factors)


def solution(mesh):
    wide = P(("gx", "gy"), None, None)
    flat = P(("gx", "gy"))
    return jax.shard_map(local, mesh=mesh, in_specs=(wide, wide, wide, flat, flat, flat, flat),
                         out_specs=(wide, wide), check_vma=False)
```

```python
import jax
import jax.numpy as jnp
from jax import lax
from jax.sharding import PartitionSpec as P
from jax.experimental import pallas as pl
from jax.experimental.pallas import tpu as pltpu

ITERS = 3
PHASES = 2 * ITERS + 1
CHUNK = 16
SLOTS = 4
UNROLL = 128
EARLY = 4


def divide(x, by):
    if by & (by - 1) == 0:
        return lax.shift_right_logical(x, by.bit_length() - 1), lax.bitwise_and(x, by - 1)
    return lax.div(x, by), lax.rem(x, by)


def kernel(len_s, count_s, source_v, target_v, count_v, em, refl, ff, sol, res,
           w, stage, runs, vt, outb, inb, dout, din, image, direction, total, rs, ds, ims,
           wout, win, want_s, ints_v, ints_s, reals_v, reals_s,
           stage_sem, send_sem, recv_sem, wsend_sem, wrecv_sem, small_sem):
    nx, ny = lax.axis_size("gx"), lax.axis_size("gy")
    n = nx * ny
    me = lax.axis_index("gx") * ny + lax.axis_index("gy")
    clusters = em.shape[0]
    blocks, cl = ff.shape[0], ff.shape[2]
    chunks = blocks // CHUNK
    f32, bf16 = jnp.float32, jnp.bfloat16

    def fetch(c, slot):
        return pltpu.make_async_copy(ff.at[pl.ds(c * CHUNK, CHUNK)], stage.at[slot], stage_sem.at[slot])

    for c in range(min(SLOTS, chunks)):
        fetch(c, c).start()

    barrier = pltpu.get_barrier_semaphore()

    i32 = jnp.int32
    lane = lax.broadcasted_iota(i32, (1, 128), 1)
    gx, gy = lax.axis_index("gx"), lax.axis_index("gy")

    def each_peer(act):
        def some(t, carry):
            for a in range(nx):
                act(lax.rem(gx + a, nx), lax.rem(gy + ny - 1 - t, ny))
            return carry

        lax.fori_loop(0, ny - 1, some, 0)
        for a in range(1, nx):
            act(lax.rem(gx + a, nx), gy)

    each_peer(lambda px, py: pl.semaphore_signal(
        barrier, inc=1, device_id=(px, py), device_id_type=pl.DeviceIdType.MESH))

    owner, slot = divide(source_v[...], clusters)
    target = target_v[...] - me * clusters
    ids = lax.broadcasted_iota(i32, (1, blocks), 1)
    peers = lax.broadcasted_iota(i32, (n, blocks), 0)
    alive = jnp.broadcast_to(ids < count_v[:, 0:1], (n, blocks))
    match = jnp.logical_and(owner == peers, alive)
    wanted = jnp.max(jnp.where(match, jnp.broadcast_to(slot, (n, blocks)), 0), axis=1, keepdims=True)
    wout[...] = jnp.broadcast_to(wanted, (n, 128)).reshape(n, 1, 128)
    pl.semaphore_wait(barrier, n - 1)

    each_peer(lambda px, py: pltpu.make_async_remote_copy(
        src_ref=wout.at[px * ny + py], dst_ref=win.at[me], send_sem=wsend_sem, recv_sem=wrecv_sem,
        device_id=(px, py), device_id_type=pl.DeviceIdType.MESH).start())
    win[me] = wout[me]

    square_of = (blocks, blocks)
    down = lax.broadcasted_iota(i32, square_of, 0)
    across = lax.broadcasted_iota(i32, square_of, 1)

    def upright(row):
        return jnp.sum(jnp.where(down == across, jnp.broadcast_to(row, square_of), 0), axis=1, keepdims=True)

    key = target * blocks + ids
    key_up, owner_up, target_up = upright(key), upright(owner), upright(target)
    rank = jnp.sum((jnp.broadcast_to(key, square_of) < key_up).astype(i32), axis=1, keepdims=True)
    placed = rank == across

    def ordered(column):
        return jnp.sum(jnp.where(placed, column, 0), axis=0, keepdims=True)

    sorted_target = ordered(jnp.broadcast_to(target_up, square_of))
    ints_v[...] = jnp.zeros(ints_v.shape, i32)
    reals_v[...] = jnp.zeros(reals_v.shape, f32)
    ints_v[0:1, :] = ordered(down)
    ints_v[1:2, :] = ordered(jnp.broadcast_to(owner_up, square_of))
    up_to = jnp.sum((target_up <= across).astype(i32), axis=0, keepdims=True)
    same = jnp.sum((target_up == across).astype(i32), axis=0, keepdims=True)
    ints_v[2:3, :] = jnp.maximum(up_to - 1, 0)
    shifted = pltpu.roll(jnp.broadcast_to(sorted_target, (8, blocks)), 1, 1)[0:1]
    joined = jnp.logical_and(shifted == sorted_target, ids > 0)
    reals_v[0:1, :] = jnp.where(joined, 1.0, 0.0)
    reals_v[1:2, :] = jnp.where(same > 0, 1.0, 0.0)
    small = (pltpu.make_async_copy(ints_v, ints_s, small_sem.at[0]),
             pltpu.make_async_copy(reals_v, reals_s, small_sem.at[1]))
    for copy in small:
        copy.start()

    def fold(pairs):
        row = jnp.zeros((1, 128), f32)
        for i, (a, b) in enumerate(pairs):
            part = jnp.sum(a[...] * b[...], axis=0)
            part = part + pltpu.roll(part, 64, 1)
            part = part + pltpu.roll(part, 32, 1)
            part = jnp.sum(part, axis=0, keepdims=True)
            row = jnp.where(lane // 32 == i, part, row)
        return row

    def send(phase, field, pairs):
        row = fold(pairs)
        if field is None:
            dout[...] = row
            din[me] = row
        else:
            inb[phase, me, 0:8] = field[want_s[me, 0, 0]]
            inb[phase, me, 8:9] = row

        def one(px, py):
            peer = px * ny + py
            if field is None:
                src, dst = dout, din.at[me]
            else:
                outb[phase, peer, 0:8] = field[want_s[peer, 0, 0]]
                outb[phase, peer, 8:9] = row
                src, dst = outb.at[phase, peer], inb.at[phase, me]
            pltpu.make_async_remote_copy(
                src_ref=src, dst_ref=dst, send_sem=send_sem.at[phase], recv_sem=recv_sem.at[phase],
                device_id=(px, py), device_id_type=pl.DeviceIdType.MESH).start()

        each_peer(one)

    def drain(ref, sem):
        part = ref.at[pl.ds(0, n - 1)]
        pltpu.make_async_copy(part, part, sem).wait()

    def receive(phase, rows):
        if rows:
            drain(inb.at[phase], recv_sem.at[phase])
            drain(outb.at[phase], send_sem.at[phase])
            return inb[phase, :, 8, :]
        drain(din, recv_sem.at[phase])
        drain(din, send_sem.at[phase])
        return din[...].reshape(n, 128)

    def whole(parts, i):
        column = jnp.sum(parts, axis=0, keepdims=True)
        return jnp.broadcast_to(
            jnp.sum(jnp.where(lane // 32 == i, column, 0.0), axis=1, keepdims=True), (8, 128))

    def put_sources(v):
        low = v - v.astype(bf16).astype(f32)
        vt[...] = jnp.concatenate([v, low], axis=1).astype(bf16)

    def apply(v):
        def step(s, acc):
            for u in range(UNROLL // 2):
                r = s * UNROLL + 2 * u
                va, vb = vt[ints_s[1, r]], vt[ints_s[1, r + 1]]
                left = jnp.concatenate([jnp.concatenate([va, va], axis=1),
                                        jnp.concatenate([vb, vb], axis=1)], axis=0)
                right = jnp.concatenate([w[ints_s[0, r]], w[ints_s[0, r + 1]]], axis=1)
                out = jnp.dot(left, right, preferred_element_type=f32)
                acc = acc * reals_s[0, r] + (out[0:8, :cl] + out[8:16, :cl])
                runs[r] = acc
                acc = acc * reals_s[0, r + 1] + (out[16:24, cl:] + out[24:32, cl:])
                runs[r + 1] = acc
            return acc

        lax.fori_loop(0, blocks // UNROLL, step, jnp.zeros((8, cl), f32))
        g = jnp.stack([runs[ints_s[2, t]] * reals_s[1, t] for t in range(clusters)])
        return v - refl[...] * g

    def prepare(c, carry):
        slot = lax.rem(c, SLOTS)
        fetch(c, slot).wait()

        def block(b, inner):
            k = c * CHUNK + b
            t = stage[slot, b].T
            j = lax.broadcasted_iota(jnp.int32, (cl, cl), 0)
            t = jnp.where(j < jnp.where(k < count_s[0], len_s[k], 0), t, 0.0)
            high = t.astype(bf16)
            w[k, 0:cl] = high
            w[k, cl:2 * cl] = (t - high.astype(f32)).astype(bf16)
            return inner

        lax.fori_loop(0, CHUNK, block, 0, unroll=4)

        @pl.when(c + SLOTS < chunks)
        def _():
            fetch(c + SLOTS, slot).start()

        return carry

    early = min(EARLY, chunks)
    lax.fori_loop(0, early, prepare, 0)
    drain(win, wrecv_sem)
    drain(wout, wsend_sem)
    asked = pltpu.make_async_copy(win, want_s, small_sem.at[2])
    asked.start()
    asked.wait()
    send(0, em, [(em, em)])
    lax.fori_loop(early, chunks, prepare, 0)
    for copy in small:
        copy.wait()

    rho = whole(receive(0, True), 0)
    rs[...] = inb[0, :, 0:8, :]
    res[...] = em[...]
    rho_old, alpha, omega = None, None, None
    for it in range(ITERS):
        last = it == ITERS - 1
        if it == 0:
            direction[...] = em[...]
            ds[...] = rs[...]
        else:
            beta = rho / rho_old * (alpha / omega)
            direction[...] = res[...] + beta * (direction[...] - omega * image[...])
            ds[...] = rs[...] + beta * (ds[...] - omega * ims[...])
        put_sources(ds[...])
        image[...] = apply(direction[...])
        phase = 1 + 2 * it
        send(phase, image, [(em, image)])
        alpha = rho / whole(receive(phase, True), 0)
        ims[...] = inb[phase, :, 0:8, :]
        res[...] = res[...] - alpha * image[...]
        rs[...] = rs[...] - alpha * ims[...]
        put_sources(rs[...])
        sol[...] = apply(res[...])
        send(phase + 1, None if last else sol, [(sol, res), (sol, sol), (em, res), (em, sol)])
        parts = receive(phase + 1, not last)
        omega = whole(parts, 0) / whole(parts, 1)
        if it == 0:
            total[...] = alpha * direction[...] + omega * res[...]
        else:
            total[...] = total[...] + alpha * direction[...] + omega * res[...]
        res[...] = res[...] - omega * sol[...]
        if not last:
            rs[...] = rs[...] - omega * inb[phase + 1, :, 0:8, :]
        rho_old = rho
        rho = whole(parts - omega[0:1] * pltpu.roll(parts, 96, 1), 2)
    sol[...] = total[...]


def local(emission, reflectance, form_factors, link_source, link_target, link_length, block_count):
    clusters, bands, cl = emission.shape
    blocks = form_factors.shape[0]
    devices = lax.axis_size(("gx", "gy"))
    i32, f32, bf16 = jnp.int32, jnp.float32, jnp.bfloat16
    smem = pl.BlockSpec(memory_space=pltpu.SMEM)
    vmem = pl.BlockSpec(memory_space=pltpu.VMEM)
    field = (clusters, bands, cl)
    rows = (devices, bands, cl)
    dma = pltpu.SemaphoreType.DMA
    return pl.pallas_call(
        kernel,
        out_shape=[jax.ShapeDtypeStruct(field, f32)] * 2,
        in_specs=[smem] * 2 + [vmem] * 5 + [pl.BlockSpec(memory_space=pl.ANY)],
        out_specs=[vmem, vmem],
        scratch_shapes=[
            pltpu.VMEM((blocks, 2 * cl, cl), bf16),
            pltpu.VMEM((SLOTS, CHUNK, cl, cl), f32),
            pltpu.VMEM((blocks, bands, cl), f32),
            pltpu.VMEM((devices, 2 * bands, cl), bf16),
            pltpu.VMEM((PHASES - 1, devices, bands + 1, cl), f32),
            pltpu.VMEM((PHASES - 1, devices, bands + 1, cl), f32),
            pltpu.VMEM((1, 128), f32),
            pltpu.VMEM((devices, 1, 128), f32),
            pltpu.VMEM(field, f32),
            pltpu.VMEM(field, f32),
            pltpu.VMEM(field, f32),
            pltpu.VMEM(rows, f32),
            pltpu.VMEM(rows, f32),
            pltpu.VMEM(rows, f32),
            pltpu.VMEM((devices, 1, 128), i32),
            pltpu.VMEM((devices, 1, 128), i32),
            pltpu.SMEM((devices, 1, 128), i32),
            pltpu.VMEM((8, blocks), i32),
            pltpu.SMEM((8, blocks), i32),
            pltpu.VMEM((8, blocks), f32),
            pltpu.SMEM((8, blocks), f32),
            dma((SLOTS,)),
            dma((PHASES,)),
            dma((PHASES,)),
            dma,
            dma,
            dma((3,)),
        ],
        compiler_params=pltpu.CompilerParams(
            collective_id=0, has_side_effects=True, vmem_limit_bytes=56 * 1024 * 1024),
        name="radiosity",
    )(link_length, block_count, link_source.reshape(1, blocks), link_target.reshape(1, blocks),
      block_count.reshape(1, 1), emission, reflectance, form_factors)


def solution(mesh):
    wide = P(("gx", "gy"), None, None)
    flat = P(("gx", "gy"))
    return jax.shard_map(local, mesh=mesh, in_specs=(wide, wide, wide, flat, flat, flat, flat),
                         out_specs=(wide, wide), check_vma=False)
```
